32 devices in a mesh: rows: 16 (over z, x, core), cols: 2 (over y).
Axes of the slice: x: 2, y: 2, z: 4, core: 2. Of those that a mesh axis runs over, the one named last changes fastest.
Arguments:
- kets: float32 [16, 4, 32], P('rows', 'cols'), may hold values from -3 to 3
- left_maps: float32 [2, 16, 4, 96, 384], P(None, 'rows', 'cols'), may hold values from -0.3125 to 0.3125
- right_maps: float32 [2, 16, 4, 96, 384], P(None, 'rows', 'cols'), may hold values from -0.3125 to 0.3125
- top_edge: float32 [4, 96, 384], P('cols'), may hold values from -6 to 6
- bottom_edge: float32 [4, 96, 384], P('cols'), may hold values from -6 to 6
- left_edge: float32 [16, 96, 384], P('rows'), may hold values from -6 to 6
- right_edge: float32 [16, 96, 384], P('rows'), may hold values from -6 to 6
- term_rows: int32 [16], replicated, may hold values from 0 to 15
- term_bonds: int32 [16], replicated, may hold values from 0 to 2
- term_ops: int32 [16], replicated, may hold values from 0 to 3
- operators: float32 [4, 16], replicated, may hold values from -6 to 6
Outputs:
- top_out: float32 [16, 4, 96, 384], P('rows', 'cols')
- bottom_out: float32 [16, 4, 96, 384], P('rows', 'cols')
- energies: float32 [16], replicated
The draws below stay inside these ranges and needn't reach their ends.
Inputs may be any that keep to these rules, and one draw needn't show every extreme that they name: Term t acts on the bond between columns term_bonds[t] and term_bonds[t] + 1 of row term_rows[t].
All inputs are finite; a program needn't handle non-finite values.
Results may differ from the reference program's by a relative error of at most 0.0003.
Values sent between devices are 32-bit elements; how exact they have to be, the bound alone decides.
A program may use at most 64 MiB of HBM per device.

```python
import jax
import jax.numpy as jnp
from jax import lax

D = 2
D2 = 4
PHYS = 2
CHI = 96
OPS = 4
TERMS = 16
NR = 16
NC = 4


def set_ends(array, rng, least, top_value):
    index_at = [jax.random.randint(jax.random.fold_in(rng, axis), (), 0, length) for axis, length in enumerate(array.shape)]
    widest = array.shape.index(max(array.shape))
    beside = index_at[:widest] + [(index_at[widest] + 1) % array.shape[widest]] + index_at[widest + 1:]
    return array.at[tuple(index_at)].set(least).at[tuple(beside)].set(top_value)


def levels(stream_key, shape, pieces, least, largest):
    factor_of = 1.0
    for axis_at, parts in pieces:
        draws = jax.random.uniform(jax.random.fold_in(jax.random.fold_in(stream_key, 6), axis_at), (parts,), jnp.float32, least / len(pieces), largest / len(pieces))
        factor_of = factor_of * jnp.repeat(jnp.exp(draws), shape[axis_at] // parts).reshape((-1,) + (1,) * (len(shape) - 1 - axis_at))
    return factor_of


def gaussian(key, dims, scale, most, shards=(), kind=jnp.bfloat16):
    entries = jax.random.normal(key, dims, jnp.float32) * scale
    if len(shards) > 0:
        entries = levels(key, dims, shards, -0.22, 0.18) * entries
    return jnp.clip(entries, min=-most, max=most).astype(kind)


def setup_inputs(seed: int = 0) -> dict:
    key_list = jax.random.split(jax.random.key(seed), 12)
    kets = gaussian(key_list[0], (NR, NC, PHYS * D**4), 0.5, 3.0, ((0, 16), (1, 2)), jnp.float32)
    left_maps = gaussian(key_list[1], (2, NR, NC, CHI, CHI * D2), (CHI * D2) ** -0.5, 0.3125, ((1, 16), (2, 2)), jnp.float32)
    right_maps = gaussian(key_list[2], (2, NR, NC, CHI, CHI * D2), (CHI * D2) ** -0.5, 0.3125, ((1, 16), (2, 2)), jnp.float32)
    top_edge = gaussian(key_list[3], (NC, CHI, D2 * CHI), 1.0, 6.0, ((0, 2),), jnp.float32)
    bottom_edge = gaussian(key_list[4], (NC, CHI, D2 * CHI), 1.0, 6.0, ((0, 2),), jnp.float32)
    left_edge = gaussian(key_list[5], (NR, CHI, D2 * CHI), 1.0, 6.0, ((0, 16),), jnp.float32)
    right_edge = gaussian(key_list[6], (NR, CHI, D2 * CHI), 1.0, 6.0, ((0, 16),), jnp.float32)
    term_rows = set_ends(jax.random.randint(key_list[7], (TERMS,), 0, NR), jax.random.fold_in(key_list[7], 1), 0, NR - 1).astype(jnp.int32)
    term_bonds = set_ends(jax.random.randint(key_list[8], (TERMS,), 0, NC - 1), jax.random.fold_in(key_list[8], 1), 0, (NC - 1) - 1).astype(jnp.int32)
    term_ops = set_ends(jax.random.randint(key_list[9], (TERMS,), 0, OPS), jax.random.fold_in(key_list[9], 1), 0, OPS - 1).astype(jnp.int32)
    operators = gaussian(key_list[10], (OPS, PHYS**4), 1.0, 6.0, (), jnp.float32)
    return dict(kets=kets, left_maps=left_maps, right_maps=right_maps, top_edge=top_edge, bottom_edge=bottom_edge, left_edge=left_edge, right_edge=right_edge, term_rows=term_rows, term_bonds=term_bonds, term_ops=term_ops, operators=operators)


EPSILON = 1e-06
PRECISION_HIGH = lax.Precision.HIGHEST

def product(pattern, former, latter):
    return jnp.einsum(pattern, former, latter, precision=PRECISION_HIGH, preferred_element_type=jnp.float32)

def normalize(values):
    return values / jnp.sqrt(jnp.mean(values * values) + EPSILON)

def select_at(values, position):
    return lax.dynamic_index_in_dim(values, position, 0, keepdims=False)

def pair_layers(ket_flat):
    tensor = ket_flat.reshape(PHYS, D, D, D, D)
    doubled = product('pabcd,pefgh->aebfcgdh', tensor, tensor)
    return doubled.reshape(D2, D2, D2, D2)

def open_layers(ket_flat):
    tensor = ket_flat.reshape(PHYS, D, D, D, D)
    doubled = product('pabcd,qefgh->pqaebfcgdh', tensor, tensor)
    return doubled.reshape(PHYS * PHYS, D2, D2, D2, D2)

def pair_diagonal():
    matched = jnp.arange(PHYS)[:, None] == jnp.arange(PHYS)[None, :]
    return jnp.where(matched, 1.0, 0.0).astype(jnp.float32).reshape(PHYS * PHYS)

def absorb_down(boundary, layers, left_map, right_map):
    above_col = boundary.reshape(CHI, D2, CHI)
    left_three = left_map.reshape(CHI, CHI, D2)
    right_three = right_map.reshape(CHI, CHI, D2)
    joined = product('aub,cbr->aurc', above_col, right_three)
    through = product('aurc,uldr->aldc', joined, layers)
    renewed = product('xal,aldc->xdc', left_three, through)
    return normalize(renewed.reshape(CHI, D2 * CHI))

def absorb_up(boundary, layers, left_map, right_map):
    below_col = boundary.reshape(CHI, D2, CHI)
    left_three = left_map.reshape(CHI, CHI, D2)
    right_three = right_map.reshape(CHI, CHI, D2)
    joined = product('adb,cbr->adrc', below_col, right_three)
    through = product('adrc,uldr->aluc', joined, layers)
    renewed = product('xal,aluc->xuc', left_three, through)
    return normalize(renewed.reshape(CHI, D2 * CHI))

def left_core(environ, layers, above_col, below_col):
    env_three = environ.reshape(CHI, D2, CHI)
    upper_three = above_col.reshape(CHI, D2, CHI)
    lower_three = below_col.reshape(CHI, D2, CHI)
    step_one = product('alb,aux->lbux', env_three, upper_three)
    step_two = product('lbux,uldr->bxdr', step_one, layers)
    return product('bxdr,bdy->xry', step_two, lower_three).reshape(CHI, D2 * CHI)

def right_core(environ, layers, above_col, below_col):
    env_three = environ.reshape(CHI, D2, CHI)
    upper_three = above_col.reshape(CHI, D2, CHI)
    lower_three = below_col.reshape(CHI, D2, CHI)
    step_one = product('xry,aux->ryau', env_three, upper_three)
    step_two = product('ryau,uldr->yald', step_one, layers)
    return product('yald,bdy->alb', step_two, lower_three).reshape(CHI, D2 * CHI)

def reference(kets, left_maps, right_maps, top_edge, bottom_edge, left_edge, right_edge, term_rows, term_bonds, term_ops, operators):
    layers = jax.vmap(jax.vmap(pair_layers))(kets)

    def down_row(carried, inputs):
        renewed = jax.vmap(absorb_down)(carried, inputs[0], inputs[1], inputs[2])
        return (renewed, renewed)

    def up_row(carried, inputs):
        renewed = jax.vmap(absorb_up)(carried, inputs[0], inputs[1], inputs[2])
        return (renewed, renewed)
    unused_top, top_out = lax.scan(down_row, top_edge, (layers, left_maps[0], right_maps[0]))
    unused_bottom, bottom_out = lax.scan(up_row, bottom_edge, (layers, left_maps[1], right_maps[1]), reverse=True)
    above = jnp.concatenate([top_edge[None], top_out[:-1]], axis=0)
    below = jnp.concatenate([bottom_out[1:], bottom_edge[None]], axis=0)
    diagonal = pair_diagonal()
    weights = jnp.outer(diagonal, diagonal).reshape(-1)

    def one_term(term_index):
        term_row = select_at(term_rows, term_index).astype(jnp.int32)
        term_bond = select_at(term_bonds, term_index).astype(jnp.int32)
        row_layers = select_at(layers, term_row)
        row_kets = select_at(kets, term_row)
        row_above = select_at(above, term_row)
        row_below = select_at(below, term_row)

        def left_walk(column, environ):
            return normalize(left_core(environ, select_at(row_layers, column), select_at(row_above, column), select_at(row_below, column)))

        def right_walk(step_count, environ):
            column = (NC - 1 - step_count).astype(jnp.int32)
            return normalize(right_core(environ, select_at(row_layers, column), select_at(row_above, column), select_at(row_below, column)))
        left_env = lax.fori_loop(0, term_bond, left_walk, select_at(left_edge, term_row))
        right_env = lax.fori_loop(0, NC - 2 - term_bond, right_walk, select_at(right_edge, term_row))
        right_col = (term_bond + 1).astype(jnp.int32)
        open_left = lax.map(lambda single: left_core(left_env, single, select_at(row_above, term_bond), select_at(row_below, term_bond)), open_layers(select_at(row_kets, term_bond)))
        open_right = lax.map(lambda single: right_core(right_env, single, select_at(row_above, right_col), select_at(row_below, right_col)), open_layers(select_at(row_kets, right_col)))
        density = product('pz,qz->pq', open_left.reshape(PHYS * PHYS, -1), open_right.reshape(PHYS * PHYS, -1)).reshape(-1)
        trace_value = jnp.sum(density * weights)
        spread = jnp.sqrt(jnp.sum(density * density))
        denominator = jnp.maximum(jnp.abs(trace_value), 0.25 * spread)
        chosen_op = select_at(operators, select_at(term_ops, term_index).astype(jnp.int32))
        return jnp.sum(density * chosen_op) / denominator
    energies = lax.map(one_term, jnp.arange(TERMS, dtype=jnp.int32))
    return (top_out, bottom_out, energies)
```

```python
import functools

import jax
import jax.numpy as jnp
from jax import lax
from jax.experimental import pallas as pl
from jax.experimental.pallas import tpu as pltpu
from jax.sharding import PartitionSpec as P

D = 2
D2 = 4
PHYS = 2
CHI = 96
OPS = 4
TERMS = 16


EPSILON = 1e-06
PRECISION_HIGH = lax.Precision.HIGH


def shifted(value, axis, steps):
    count = lax.axis_size(axis)
    initial, last = (max(0, -steps), min(count, count - steps))
    return lax.ppermute(value, axis, [(source, source + steps) for source in range(initial, last)])


def product(pattern, former, latter):
    return jnp.einsum(
        pattern, former, latter, precision=PRECISION_HIGH, preferred_element_type=jnp.float32
    )


def normalize(values):
    return values / jnp.sqrt(jnp.mean(values * values) + EPSILON)


def select_at(values, position):
    return lax.dynamic_index_in_dim(values, position, 0, keepdims=False)


def pair_layers(ket_flat):
    tensor = ket_flat.reshape(PHYS, D, D, D, D)
    doubled = product("pabcd,pefgh->aebfcgdh", tensor, tensor)
    return doubled.reshape(D2, D2, D2, D2)


def open_layers(ket_flat):
    tensor = ket_flat.reshape(PHYS, D, D, D, D)
    doubled = product("pabcd,qefgh->pqaebfcgdh", tensor, tensor)
    return doubled.reshape(PHYS * PHYS, D2, D2, D2, D2)


def pair_diagonal():
    matched = jnp.arange(PHYS)[:, None] == jnp.arange(PHYS)[None, :]
    return jnp.where(matched, 1.0, 0.0).astype(jnp.float32).reshape(PHYS * PHYS)


def left_core(environ, layers, above_col, below_col):
    env_three = environ.reshape(CHI, D2, CHI)
    upper_three = above_col.reshape(CHI, D2, CHI)
    lower_three = below_col.reshape(CHI, D2, CHI)
    step_one = product("alb,aux->lbux", env_three, upper_three)
    step_two = product("lbux,uldr->bxdr", step_one, layers)
    return product("bxdr,bdy->xry", step_two, lower_three).reshape(CHI, D2 * CHI)


def right_core(environ, layers, above_col, below_col):
    env_three = environ.reshape(CHI, D2, CHI)
    upper_three = above_col.reshape(CHI, D2, CHI)
    lower_three = below_col.reshape(CHI, D2, CHI)
    step_one = product("xry,aux->ryau", env_three, upper_three)
    step_two = product("ryau,uldr->yald", step_one, layers)
    return product("yald,bdy->alb", step_two, lower_three).reshape(CHI, D2 * CHI)


def side_step(core_map, environ, ket_flat, layers, above_col, below_col, wanted):

    def with_open(unused):
        opened = lax.map(
            lambda single: core_map(environ, single, above_col, below_col), open_layers(ket_flat)
        )
        closed = jnp.sum(pair_diagonal()[:, None, None] * opened, axis=0)
        return (opened, normalize(closed))

    def without_open(unused):
        empty_open = jnp.zeros((PHYS * PHYS, CHI, D2 * CHI), jnp.float32)
        return (empty_open, normalize(core_map(environ, layers, above_col, below_col)))

    return lax.cond(wanted, with_open, without_open, 0)


LANES = 128


def unpack_lanes(tiles, chi):
    rolled = {}
    lane = lax.broadcasted_iota(jnp.int32, tiles[0].shape, 1)
    blocks = []
    for block in range(D2):
        total = jnp.zeros_like(tiles[0])
        for place, tile in enumerate(tiles):
            low = max(chi * block, LANES * place)
            high = min(chi * (block + 1), LANES * (place + 1))
            if low >= high:
                continue
            shift = (LANES * place - chi * block) % LANES
            if (place, shift) not in rolled:
                rolled[place, shift] = tile if shift == 0 else pltpu.roll(tile, shift, 1)
            inside = (lane >= low - chi * block) & (lane < high - chi * block)
            total = jnp.where(inside, rolled[place, shift], total)
        blocks.append(total)
    return blocks


def pack_lanes(blocks, chi):
    lane = lax.broadcasted_iota(jnp.int32, blocks[0].shape, 1)
    rolled = {}
    tiles = []
    for place in range(chi * D2 // LANES):
        total = jnp.zeros_like(blocks[0])
        for block, values in enumerate(blocks):
            low = max(chi * block, LANES * place)
            high = min(chi * (block + 1), LANES * (place + 1))
            if low >= high:
                continue
            shift = (chi * block - LANES * place) % LANES
            if (block, shift) not in rolled:
                rolled[block, shift] = values if shift == 0 else pltpu.roll(values, shift, 1)
            inside = (lane >= low - LANES * place) & (lane < high - LANES * place)
            total = jnp.where(inside, rolled[block, shift], total)
        tiles.append(total)
    return tiles


def halves(values):
    high = values.astype(jnp.bfloat16)
    low = (values - high.astype(jnp.float32)).astype(jnp.bfloat16)
    return high, low


def dot32(former, latter):
    return jnp.dot(former, latter, preferred_element_type=jnp.float32)


def dot_last(former, latter):
    return lax.dot_general(
        former, latter, (((1,), (1,)), ((), ())), preferred_element_type=jnp.float32
    )


def load_tiles(ref, at, width):
    return [ref[at, :, LANES * t : LANES * (t + 1)] for t in range(width // LANES)]


def chain_kernel(
    row_count,
    kets_ref,
    left_ref,
    right_ref,
    top_ref,
    bottom_ref,
    out_ref,
    env_ref,
    pbuf,
    qbuf,
    kbuf,
    xbuf,
    ebuf,
    pick,
    phi,
    plo,
    qhi,
    qlo,
    x32,
    jbuf,
    thi,
    tlo,
    map_send,
    map_recv,
    env_send,
    env_recv,
    out_send,
    out_recv,
    hop_send,
    hop_recv,
):
    local_cols = kets_ref.shape[1]
    chi, width = left_ref.shape[2], left_ref.shape[3]
    group = 2 * local_cols
    groups = row_count // group
    place = lax.axis_index("rows")
    mine = place // group
    me = place % group
    column = me // 2
    way = me % 2
    base = mine * group
    before = mine - 1 + 2 * way
    after = mine + 1 - 2 * way
    has_before = (before >= 0) & (before < groups)
    has_after = (after >= 0) & (after < groups)

    barrier = pltpu.get_barrier_semaphore()
    for other in range(group):

        @pl.when(me != other)
        def _():
            pl.semaphore_signal(barrier, inc=1, device_id={"rows": base + other})

    @pl.when(has_before)
    def _():
        pl.semaphore_signal(barrier, inc=1, device_id={"rows": before * group + me})

    @pl.when(has_after)
    def _():
        pl.semaphore_signal(barrier, inc=1, device_id={"rows": after * group + me})

    waits = group - 1 + jnp.where(has_before, 1, 0) + jnp.where(has_after, 1, 0)
    pl.semaphore_wait(barrier, waits)

    def map_copies(target_way, target_col, target, local):
        made = []
        for kind, (source, buffer) in enumerate(
            ((kets_ref, kbuf), (right_ref, qbuf), (left_ref, pbuf))
        ):
            origin, landing = source.at[target_way, target_col], buffer.at[me]
            if local:
                made.append(pltpu.make_async_copy(origin, landing, map_recv.at[kind, me]))
            else:
                made.append(
                    pltpu.make_async_remote_copy(
                        origin,
                        landing,
                        map_send.at[kind, target],
                        map_recv.at[kind, me],
                        device_id={"rows": base + target},
                    )
                )
        return made

    late = jnp.where(mine >= groups // 2, 1, 0)
    for turn in range(group):
        target_way = (late + turn // local_cols) % 2
        target_col = turn % local_cols
        target = target_col * 2 + target_way

        @pl.when(target != me)
        def _():
            for copy in map_copies(target_way, target_col, target, False):
                copy.start()

        @pl.when(target == me)
        def _():
            for copy in map_copies(target_way, target_col, target, True):
                copy.start()

    chosen = lax.broadcasted_iota(jnp.int32, (D2 * LANES, width), 0)
    entry = lax.broadcasted_iota(jnp.int32, (D2 * LANES, width), 1)
    wanted = (chosen % LANES) * D2 + chosen // LANES
    live = (chosen % LANES) < chi
    pick[...] = jnp.where((wanted == entry) & live, 1.0, 0.0).astype(jnp.bfloat16)
    thi[...] = jnp.zeros_like(thi)
    tlo[...] = jnp.zeros_like(tlo)

    def prepare(step, unused):
        slot = step + way * (group - 1 - 2 * step)
        for kind, buffer in enumerate((kbuf, qbuf, pbuf)):
            pltpu.make_async_copy(
                buffer.at[slot], buffer.at[slot], map_recv.at[kind, slot]
            ).wait()
        ket = kbuf[slot]
        half = ket.shape[0] // PHYS
        for i in range(half):
            total = ket[i : i + 1] * ket[0:half]
            for p in range(1, PHYS):
                total += ket[p * half + i : p * half + i + 1] * ket[p * half : (p + 1) * half]
            ebuf[step, i * half : (i + 1) * half] = total
        values = pick[...]
        for source, high_ref, low_ref, right in (
            (qbuf, qhi, qlo, True),
            (pbuf, phi, plo, False),
        ):
            for part, ref in zip(halves(source[slot]), (high_ref, low_ref)):
                if right:
                    fill = jnp.zeros((LANES - chi, width), jnp.bfloat16)
                    tall = dot_last(values, jnp.concatenate([part, fill], axis=0))
                    for w in range(D2):
                        ref[step, :, w * LANES : (w + 1) * LANES] = tall[
                            w * LANES : (w + 1) * LANES
                        ].astype(jnp.bfloat16)
                else:
                    ref[step] = dot_last(part, values).astype(jnp.bfloat16)
        return unused

    def row_copy(source, landing, send, recv, slot):
        remote = pltpu.make_async_remote_copy(
            source, landing, send, recv, device_id={"rows": base + slot}
        )
        return remote, pltpu.make_async_copy(source, landing, recv)

    def send_row(source, landing, send, recv, slot):
        remote, local = row_copy(source, landing, send, recv, slot)

        @pl.when(slot != me)
        def _():
            remote.start()

        @pl.when(slot == me)
        def _():
            local.start()

    hop = pltpu.make_async_remote_copy(
        xbuf.at[group],
        xbuf.at[0],
        hop_send,
        hop_recv,
        device_id={"rows": after * group + me},
    )

    ahead = jnp.where(has_before, group, 1)
    lax.fori_loop(0, ahead, prepare, 0)

    @pl.when(has_before)
    def _():
        pltpu.make_async_copy(xbuf.at[0], xbuf.at[0], hop_recv).wait()

    @pl.when(jnp.logical_not(has_before) & (way == 0))
    def _():
        xbuf[0] = top_ref[column]

    @pl.when(jnp.logical_not(has_before) & (way == 1))
    def _():
        xbuf[0] = bottom_ref[column]

    for u, block in enumerate(unpack_lanes(load_tiles(xbuf, 0, width), chi)):
        x32[u * chi : (u + 1) * chi] = block

    def absorb(step, unused):
        slot = step + way * (group - 1 - 2 * step)

        @pl.when(step >= ahead)
        def _():
            prepare(step, 0)

        send_row(
            xbuf.at[step], env_ref.at[way, column], env_send.at[step], env_recv.at[way, column], slot
        )
        x_high, x_low = halves(x32[...])
        q_high = qhi[step]
        jbuf[...] = dot32(x_high, q_high) + (dot32(x_high, qlo[step]) + dot32(x_low, q_high))
        chunk = 16

        def through(at, unused):
            start = pl.multiple_of(at * chunk, chunk)
            for l in range(D2):
                for d in range(D2):
                    total = None
                    for u in range(D2):
                        for w in range(D2):
                            ket_at = (u // D) * 8 + (l // D) * 4 + (d // D) * 2 + w // D
                            bra_at = (u % D) * 8 + (l % D) * 4 + (d % D) * 2 + w % D
                            spot = ket_at * 16 + bra_at
                            term = (
                                ebuf[step, spot : spot + 1, :]
                                * jbuf[
                                    pl.ds(u * chi + start, chunk), w * LANES : (w + 1) * LANES
                                ]
                            )
                            total = term if total is None else total + term
                    high, low = halves(total)
                    rows = pl.ds(l * LANES + start, chunk)
                    thi[rows, d * LANES : (d + 1) * LANES] = high
                    tlo[rows, d * LANES : (d + 1) * LANES] = low
            return unused

        lax.fori_loop(0, chi // chunk, through, 0)
        t_high = thi[...]
        p_high = phi[step]
        renewed = dot32(p_high, t_high) + (dot32(p_high, tlo[...]) + dot32(plo[step], t_high))
        square = jnp.sum(jnp.sum(renewed * renewed, axis=1, keepdims=True), axis=0, keepdims=True)
        renewed = renewed * (1.0 / jnp.sqrt(square / (chi * width) + EPSILON))
        blocks = [renewed[:, d * LANES : (d + 1) * LANES] for d in range(D2)]
        for d, block in enumerate(blocks):
            x32[d * chi : (d + 1) * chi] = block
        for t, tile in enumerate(pack_lanes(blocks, chi)):
            xbuf[step + 1, :, t * LANES : (t + 1) * LANES] = tile

        @pl.when((step == group - 1) & has_after)
        def _():
            hop.start()

        send_row(
            xbuf.at[step + 1],
            out_ref.at[way, column],
            out_send.at[step],
            out_recv.at[way, column],
            slot,
        )
        return unused

    lax.fori_loop(0, group, absorb, 0)

    for step in range(group):
        slot = step + way * (group - 1 - 2 * step)

        @pl.when(slot != me)
        def _():
            row_copy(
                xbuf.at[step],
                env_ref.at[way, column],
                env_send.at[step],
                env_recv.at[way, column],
                slot,
            )[0].wait_send()
            row_copy(
                xbuf.at[step + 1],
                out_ref.at[way, column],
                out_send.at[step],
                out_recv.at[way, column],
                slot,
            )[0].wait_send()

    for target in range(group):

        @pl.when(target != me)
        def _():
            for copy in map_copies(target % 2, target // 2, target, False):
                copy.wait_send()

    @pl.when(has_after)
    def _():
        hop.wait_send()

    for a in range(2):
        for b in range(local_cols):
            pltpu.make_async_copy(env_ref.at[a, b], env_ref.at[a, b], env_recv.at[a, b]).wait()
            pltpu.make_async_copy(out_ref.at[a, b], out_ref.at[a, b], out_recv.at[a, b]).wait()


def boundary_chains(row_count, kets, left_maps, right_maps, top_edge, bottom_edge):
    local_cols = kets.shape[1]
    chi, width = left_maps.shape[-2:]
    group = 2 * local_cols
    tensors = kets[0].reshape((local_cols, PHYS) + (D,) * 4)
    both = jnp.stack([tensors, jnp.swapaxes(tensors, 2, 4)]).reshape(2, local_cols, -1)
    spread = jnp.broadcast_to(both[..., None], both.shape + (LANES,))
    shape = jax.ShapeDtypeStruct((2, local_cols, chi, width), jnp.float32)
    vmem = pl.BlockSpec(memory_space=pltpu.VMEM)
    wide = D2 * LANES
    dma = pltpu.SemaphoreType.DMA
    return pl.pallas_call(
        functools.partial(chain_kernel, row_count),
        out_shape=(shape, shape),
        in_specs=[vmem] * 5,
        out_specs=(vmem, vmem),
        scratch_shapes=[
            pltpu.VMEM((group, chi, width), jnp.float32),
            pltpu.VMEM((group, chi, width), jnp.float32),
            pltpu.VMEM((group,) + spread.shape[2:], jnp.float32),
            pltpu.VMEM((group + 1, chi, width), jnp.float32),
            pltpu.VMEM((group, D2**4, LANES), jnp.float32),
            pltpu.VMEM((wide, width), jnp.bfloat16),
            pltpu.VMEM((group, chi, wide), jnp.bfloat16),
            pltpu.VMEM((group, chi, wide), jnp.bfloat16),
            pltpu.VMEM((group, LANES, wide), jnp.bfloat16),
            pltpu.VMEM((group, LANES, wide), jnp.bfloat16),
            pltpu.VMEM((D2 * chi, LANES), jnp.float32),
            pltpu.VMEM((D2 * chi, wide), jnp.float32),
            pltpu.VMEM((wide, wide), jnp.bfloat16),
            pltpu.VMEM((wide, wide), jnp.bfloat16),
            dma((3, group)),
            dma((3, group)),
            dma((group,)),
            dma((2, local_cols)),
            dma((group,)),
            dma((2, local_cols)),
            dma,
            dma,
        ],
        compiler_params=pltpu.CompilerParams(
            collective_id=0, has_side_effects=True, vmem_limit_bytes=48 * 1024 * 1024
        ),
        name="chains",
    )(spread, left_maps[:, 0], right_maps[:, 0], top_edge, bottom_edge)


def shards(
    kets,
    left_maps,
    right_maps,
    top_edge,
    bottom_edge,
    left_edge,
    right_edge,
    term_rows,
    term_bonds,
    term_ops,
    operators,
):
    row_count = lax.axis_size("rows")
    row_place = lax.axis_index("rows")
    col_count = lax.axis_size("cols")
    col_place = lax.axis_index("cols")
    local_rows = kets.shape[0]
    local_cols = kets.shape[1]
    layers = jax.vmap(jax.vmap(pair_layers))(kets)
    column_shape = (CHI, D2 * CHI)
    outs, envs = boundary_chains(row_count, kets, left_maps, right_maps, top_edge, bottom_edge)
    leave_top, leave_bottom = outs[0][None], outs[1][None]
    above, below = envs[0][None], envs[1][None]
    global_rows = row_place * local_rows + jnp.arange(local_rows, dtype=jnp.int32)
    global_cols = col_place * local_cols + jnp.arange(local_cols, dtype=jnp.int32)
    row_match = term_rows[:, None] == global_rows[None, :]
    site_match = row_match[:, :, None] & (term_bonds[:, None, None] == global_cols[None, None, :])
    left_need = jnp.any(site_match, axis=0)
    right_need = jnp.any(
        row_match[:, :, None] & (term_bonds[:, None, None] == global_cols[None, None, :] - 1),
        axis=0,
    )
    rows_shape = (local_rows,) + column_shape
    edge_shape = (local_rows, PHYS * PHYS) + column_shape
    open_shape = (local_rows, local_cols, PHYS * PHYS) + column_shape

    def chain_step(section_number, carried):
        from_left, from_right, edge_in, left_opens, right_opens, edge_open = carried

        def left_live(stores):
            source = jnp.where(col_place == 0, left_edge, from_left)
            environ = source[0]
            row_open = []
            for column in range(local_cols):
                opened, environ = side_step(
                    left_core,
                    environ,
                    kets[0, column],
                    layers[0, column],
                    above[0, column],
                    below[0, column],
                    left_need[0, column],
                )
                row_open.append(opened)
            opened_rows = [jnp.stack(row_open)]
            sent_rows = [environ]
            return (jnp.stack(opened_rows), jnp.stack(sent_rows))

        def left_spare(stores):
            return (stores, jnp.zeros(rows_shape, jnp.float32))

        left_opens, sent_left = lax.cond(
            section_number == col_place, left_live, left_spare, left_opens
        )

        def right_live(stores):
            source = jnp.where(col_place == col_count - 1, right_edge, from_right)
            environ = source[0]
            row_open = [None] * local_cols
            for column in reversed(range(local_cols)):
                opened, environ = side_step(
                    right_core,
                    environ,
                    kets[0, column],
                    layers[0, column],
                    above[0, column],
                    below[0, column],
                    right_need[0, column],
                )
                row_open[column] = opened
            opened_rows = [jnp.stack(row_open)]
            sent_rows = [environ]
            kept_edge = stores[1]
            return (jnp.stack(opened_rows), kept_edge, jnp.stack(sent_rows))

        def right_spare(stores):
            return (stores[0], stores[1], jnp.zeros(rows_shape, jnp.float32))

        right_opens, edge_open, sent_right = lax.cond(
            section_number == col_count - 1 - col_place,
            right_live,
            right_spare,
            (right_opens, edge_open),
        )
        from_left = shifted(sent_left, "cols", 1)
        from_right = shifted(sent_right, "cols", -1)
        return (from_left, from_right, edge_in, left_opens, right_opens, edge_open)

    chain_start = (
        jnp.zeros(rows_shape, jnp.float32),
        jnp.zeros(rows_shape, jnp.float32),
        jnp.zeros(edge_shape, jnp.float32),
        jnp.zeros(open_shape, jnp.float32),
        jnp.zeros(open_shape, jnp.float32),
        jnp.zeros(edge_shape, jnp.float32),
    )
    unused_left, unused_right, unused_edge, left_opens, right_opens, edge_open = lax.fori_loop(
        0, col_count, chain_step, chain_start
    )
    edge_open = shifted(right_opens[:, 0], "cols", -1)
    partner = jnp.concatenate([right_opens[:, 1:], edge_open[:, None]], axis=1)
    flat_left = left_opens.reshape(local_rows * local_cols, PHYS * PHYS, -1)
    flat_right = partner.reshape(local_rows * local_cols, PHYS * PHYS, -1)
    density = product("kpz,kqz->kpq", flat_left, flat_right).reshape(local_rows * local_cols, -1)
    diagonal = pair_diagonal()
    weights = jnp.outer(diagonal, diagonal).reshape(-1)
    trace_value = jnp.sum(density * weights[None, :], axis=1)
    spread = jnp.sqrt(jnp.sum(density * density, axis=1))
    valid_bond = left_need.reshape(-1)
    denominator = jnp.where(valid_bond, jnp.maximum(jnp.abs(trace_value), 0.25 * spread), 1.0)
    scaled = density / denominator[:, None]
    chooser = jnp.where(site_match.reshape(TERMS, -1), 1.0, 0.0).astype(jnp.float32)
    chosen = jnp.dot(chooser, scaled, precision=PRECISION_HIGH, preferred_element_type=jnp.float32)
    op_match = jnp.where(
        term_ops[:, None] == jnp.arange(OPS, dtype=jnp.int32)[None, :], 1.0, 0.0
    ).astype(jnp.float32)
    picked = jnp.dot(
        op_match, operators, precision=PRECISION_HIGH, preferred_element_type=jnp.float32
    )
    term_share = jnp.sum(chosen * picked, axis=1)
    energies = lax.psum(term_share, ("rows", "cols"))
    return (leave_top, leave_bottom, energies)


def solution(mesh):
    placed = (
        P("rows", "cols", None),
        P(None, "rows", "cols", None, None),
        P(None, "rows", "cols", None, None),
        P("cols", None, None),
        P("cols", None, None),
        P("rows", None, None),
        P("rows", None, None),
        P(),
        P(),
        P(),
        P(),
    )
    return jax.shard_map(
        shards,
        mesh=mesh,
        in_specs=placed,
        out_specs=(P("rows", "cols", None, None), P("rows", "cols", None, None), P()),
        check_vma=False,
    )
```

```python
import functools

import jax
import jax.numpy as jnp
from jax import lax
from jax.experimental import pallas as pl
from jax.experimental.pallas import tpu as pltpu
from jax.sharding import PartitionSpec as P

D = 2
D2 = 4
PHYS = 2
CHI = 96
OPS = 4
TERMS = 16


EPSILON = 1e-06


LANES = 128


def unpack_lanes(tiles, chi):
    rolled = {}
    lane = lax.broadcasted_iota(jnp.int32, tiles[0].shape, 1)
    blocks = []
    for block in range(D2):
        total = jnp.zeros_like(tiles[0])
        for place, tile in enumerate(tiles):
            low = max(chi * block, LANES * place)
            high = min(chi * (block + 1), LANES * (place + 1))
            if low >= high:
                continue
            shift = (LANES * place - chi * block) % LANES
            if (place, shift) not in rolled:
                rolled[place, shift] = tile if shift == 0 else pltpu.roll(tile, shift, 1)
            inside = (lane >= low - chi * block) & (lane < high - chi * block)
            total = jnp.where(inside, rolled[place, shift], total)
        blocks.append(total)
    return blocks


def pack_lanes(blocks, chi):
    lane = lax.broadcasted_iota(jnp.int32, blocks[0].shape, 1)
    rolled = {}
    tiles = []
    for place in range(chi * D2 // LANES):
        total = jnp.zeros_like(blocks[0])
        for block, values in enumerate(blocks):
            low = max(chi * block, LANES * place)
            high = min(chi * (block + 1), LANES * (place + 1))
            if low >= high:
                continue
            shift = (chi * block - LANES * place) % LANES
            if (block, shift) not in rolled:
                rolled[block, shift] = values if shift == 0 else pltpu.roll(values, shift, 1)
            inside = (lane >= low - LANES * place) & (lane < high - LANES * place)
            total = jnp.where(inside, rolled[block, shift], total)
        tiles.append(total)
    return tiles


def halves(values):
    high = values.astype(jnp.bfloat16)
    low = (values - high.astype(jnp.float32)).astype(jnp.bfloat16)
    return high, low


def dot32(former, latter):
    return jnp.dot(former, latter, preferred_element_type=jnp.float32)


def dot_last(former, latter):
    return lax.dot_general(
        former, latter, (((1,), (1,)), ((), ())), preferred_element_type=jnp.float32
    )


def load_tiles(ref, at, width):
    return [ref[at, :, LANES * t : LANES * (t + 1)] for t in range(width // LANES)]


def chain_kernel(
    row_count,
    kets_ref,
    left_ref,
    right_ref,
    top_ref,
    bottom_ref,
    out_ref,
    env_ref,
    pbuf,
    qbuf,
    kbuf,
    xbuf,
    ebuf,
    pick,
    phi,
    plo,
    qhi,
    qlo,
    x32,
    jbuf,
    thi,
    tlo,
    map_send,
    map_recv,
    env_send,
    env_recv,
    out_send,
    out_recv,
    hop_send,
    hop_recv,
):
    local_cols = kets_ref.shape[1]
    chi, width = left_ref.shape[2], left_ref.shape[3]
    group = 2 * local_cols
    groups = row_count // group
    place = lax.axis_index("rows")
    mine = place // group
    me = place % group
    column = me // 2
    way = me % 2
    base = mine * group
    before = mine - 1 + 2 * way
    after = mine + 1 - 2 * way
    has_before = (before >= 0) & (before < groups)
    has_after = (after >= 0) & (after < groups)

    barrier = pltpu.get_barrier_semaphore()
    for other in range(group):

        @pl.when(me != other)
        def _():
            pl.semaphore_signal(barrier, inc=1, device_id={"rows": base + other})

    @pl.when(has_before)
    def _():
        pl.semaphore_signal(barrier, inc=1, device_id={"rows": before * group + me})

    @pl.when(has_after)
    def _():
        pl.semaphore_signal(barrier, inc=1, device_id={"rows": after * group + me})

    waits = group - 1 + jnp.where(has_before, 1, 0) + jnp.where(has_after, 1, 0)
    pl.semaphore_wait(barrier, waits)

    def map_copies(target_way, target_col, target, local):
        made = []
        for kind, (source, buffer) in enumerate(
            ((kets_ref, kbuf), (right_ref, qbuf), (left_ref, pbuf))
        ):
            origin, landing = source.at[target_way, target_col], buffer.at[me]
            if local:
                made.append(pltpu.make_async_copy(origin, landing, map_recv.at[kind, me]))
            else:
                made.append(
                    pltpu.make_async_remote_copy(
                        origin,
                        landing,
                        map_send.at[kind, target],
                        map_recv.at[kind, me],
                        device_id={"rows": base + target},
                    )
                )
        return made

    late = jnp.where(mine >= groups // 2, 1, 0)
    for turn in range(group):
        target_way = (late + turn // local_cols) % 2
        target_col = turn % local_cols
        target = target_col * 2 + target_way

        @pl.when(target != me)
        def _():
            for copy in map_copies(target_way, target_col, target, False):
                copy.start()

        @pl.when(target == me)
        def _():
            for copy in map_copies(target_way, target_col, target, True):
                copy.start()

    chosen = lax.broadcasted_iota(jnp.int32, (D2 * LANES, width), 0)
    entry = lax.broadcasted_iota(jnp.int32, (D2 * LANES, width), 1)
    wanted = (chosen % LANES) * D2 + chosen // LANES
    live = (chosen % LANES) < chi
    pick[...] = jnp.where((wanted == entry) & live, 1.0, 0.0).astype(jnp.bfloat16)
    thi[...] = jnp.zeros_like(thi)
    tlo[...] = jnp.zeros_like(tlo)

    def prepare(step, unused):
        slot = step + way * (group - 1 - 2 * step)
        for kind, buffer in enumerate((kbuf, qbuf, pbuf)):
            pltpu.make_async_copy(
                buffer.at[slot], buffer.at[slot], map_recv.at[kind, slot]
            ).wait()
        ket = kbuf[slot]
        half = ket.shape[0] // PHYS
        for i in range(half):
            total = ket[i : i + 1] * ket[0:half]
            for p in range(1, PHYS):
                total += ket[p * half + i : p * half + i + 1] * ket[p * half : (p + 1) * half]
            ebuf[step, i * half : (i + 1) * half] = total
        values = pick[...]
        for source, high_ref, low_ref, right in (
            (qbuf, qhi, qlo, True),
            (pbuf, phi, plo, False),
        ):
            for part, ref in zip(halves(source[slot]), (high_ref, low_ref)):
                if right:
                    fill = jnp.zeros((LANES - chi, width), jnp.bfloat16)
                    tall = dot_last(values, jnp.concatenate([part, fill], axis=0))
                    for w in range(D2):
                        ref[step, :, w * LANES : (w + 1) * LANES] = tall[
                            w * LANES : (w + 1) * LANES
                        ].astype(jnp.bfloat16)
                else:
                    ref[step] = dot_last(part, values).astype(jnp.bfloat16)
        return unused

    def row_copy(source, landing, send, recv, slot):
        remote = pltpu.make_async_remote_copy(
            source, landing, send, recv, device_id={"rows": base + slot}
        )
        return remote, pltpu.make_async_copy(source, landing, recv)

    def send_row(source, landing, send, recv, slot):
        remote, local = row_copy(source, landing, send, recv, slot)

        @pl.when(slot != me)
        def _():
            remote.start()

        @pl.when(slot == me)
        def _():
            local.start()

    hop = pltpu.make_async_remote_copy(
        xbuf.at[group],
        xbuf.at[0],
        hop_send,
        hop_recv,
        device_id={"rows": after * group + me},
    )

    ahead = jnp.where(has_before, group, 1)
    lax.fori_loop(0, ahead, prepare, 0)

    @pl.when(has_before)
    def _():
        pltpu.make_async_copy(xbuf.at[0], xbuf.at[0], hop_recv).wait()

    @pl.when(jnp.logical_not(has_before) & (way == 0))
    def _():
        xbuf[0] = top_ref[column]

    @pl.when(jnp.logical_not(has_before) & (way == 1))
    def _():
        xbuf[0] = bottom_ref[column]

    for u, block in enumerate(unpack_lanes(load_tiles(xbuf, 0, width), chi)):
        x32[u * chi : (u + 1) * chi] = block

    def absorb(step, unused):
        slot = step + way * (group - 1 - 2 * step)

        @pl.when(step >= ahead)
        def _():
            prepare(step, 0)

        send_row(
            xbuf.at[step], env_ref.at[way, column], env_send.at[step], env_recv.at[way, column], slot
        )
        x_high, x_low = halves(x32[...])
        q_high = qhi[step]
        jbuf[...] = dot32(x_high, q_high) + (dot32(x_high, qlo[step]) + dot32(x_low, q_high))
        chunk = 16

        def through(at, unused):
            start = pl.multiple_of(at * chunk, chunk)
            for l in range(D2):
                for d in range(D2):
                    total = None
                    for u in range(D2):
                        for w in range(D2):
                            ket_at = (u // D) * 8 + (l // D) * 4 + (d // D) * 2 + w // D
                            bra_at = (u % D) * 8 + (l % D) * 4 + (d % D) * 2 + w % D
                            spot = ket_at * 16 + bra_at
                            term = (
                                ebuf[step, spot : spot + 1, :]
                                * jbuf[
                                    pl.ds(u * chi + start, chunk), w * LANES : (w + 1) * LANES
                                ]
                            )
                            total = term if total is None else total + term
                    high, low = halves(total)
                    rows = pl.ds(l * LANES + start, chunk)
                    thi[rows, d * LANES : (d + 1) * LANES] = high
                    tlo[rows, d * LANES : (d + 1) * LANES] = low
            return unused

        lax.fori_loop(0, chi // chunk, through, 0)
        t_high = thi[...]
        p_high = phi[step]
        renewed = dot32(p_high, t_high) + (dot32(p_high, tlo[...]) + dot32(plo[step], t_high))
        square = jnp.sum(jnp.sum(renewed * renewed, axis=1, keepdims=True), axis=0, keepdims=True)
        renewed = renewed * (1.0 / jnp.sqrt(square / (chi * width) + EPSILON))
        blocks = [renewed[:, d * LANES : (d + 1) * LANES] for d in range(D2)]
        for d, block in enumerate(blocks):
            x32[d * chi : (d + 1) * chi] = block
        for t, tile in enumerate(pack_lanes(blocks, chi)):
            xbuf[step + 1, :, t * LANES : (t + 1) * LANES] = tile

        @pl.when((step == group - 1) & has_after)
        def _():
            hop.start()

        send_row(
            xbuf.at[step + 1],
            out_ref.at[way, column],
            out_send.at[step],
            out_recv.at[way, column],
            slot,
        )
        return unused

    lax.fori_loop(0, group, absorb, 0)

    for step in range(group):
        slot = step + way * (group - 1 - 2 * step)

        @pl.when(slot != me)
        def _():
            row_copy(
                xbuf.at[step],
                env_ref.at[way, column],
                env_send.at[step],
                env_recv.at[way, column],
                slot,
            )[0].wait_send()
            row_copy(
                xbuf.at[step + 1],
                out_ref.at[way, column],
                out_send.at[step],
                out_recv.at[way, column],
                slot,
            )[0].wait_send()

    for target in range(group):

        @pl.when(target != me)
        def _():
            for copy in map_copies(target % 2, target // 2, target, False):
                copy.wait_send()

    @pl.when(has_after)
    def _():
        hop.wait_send()

    for a in range(2):
        for b in range(local_cols):
            pltpu.make_async_copy(env_ref.at[a, b], env_ref.at[a, b], env_recv.at[a, b]).wait()
            pltpu.make_async_copy(out_ref.at[a, b], out_ref.at[a, b], out_recv.at[a, b]).wait()


def boundary_chains(row_count, kets, left_maps, right_maps, top_edge, bottom_edge):
    local_cols = kets.shape[1]
    chi, width = left_maps.shape[-2:]
    group = 2 * local_cols
    tensors = kets[0].reshape((local_cols, PHYS) + (D,) * 4)
    both = jnp.stack([tensors, jnp.swapaxes(tensors, 2, 4)]).reshape(2, local_cols, -1)
    spread = jnp.broadcast_to(both[..., None], both.shape + (LANES,))
    shape = jax.ShapeDtypeStruct((2, local_cols, chi, width), jnp.float32)
    vmem = pl.BlockSpec(memory_space=pltpu.VMEM)
    wide = D2 * LANES
    dma = pltpu.SemaphoreType.DMA
    return pl.pallas_call(
        functools.partial(chain_kernel, row_count),
        out_shape=(shape, shape),
        in_specs=[vmem] * 5,
        out_specs=(vmem, vmem),
        scratch_shapes=[
            pltpu.VMEM((group, chi, width), jnp.float32),
            pltpu.VMEM((group, chi, width), jnp.float32),
            pltpu.VMEM((group,) + spread.shape[2:], jnp.float32),
            pltpu.VMEM((group + 1, chi, width), jnp.float32),
            pltpu.VMEM((group, D2**4, LANES), jnp.float32),
            pltpu.VMEM((wide, width), jnp.bfloat16),
            pltpu.VMEM((group, chi, wide), jnp.bfloat16),
            pltpu.VMEM((group, chi, wide), jnp.bfloat16),
            pltpu.VMEM((group, LANES, wide), jnp.bfloat16),
            pltpu.VMEM((group, LANES, wide), jnp.bfloat16),
            pltpu.VMEM((D2 * chi, LANES), jnp.float32),
            pltpu.VMEM((D2 * chi, wide), jnp.float32),
            pltpu.VMEM((wide, wide), jnp.bfloat16),
            pltpu.VMEM((wide, wide), jnp.bfloat16),
            dma((3, group)),
            dma((3, group)),
            dma((group,)),
            dma((2, local_cols)),
            dma((group,)),
            dma((2, local_cols)),
            dma,
            dma,
        ],
        compiler_params=pltpu.CompilerParams(
            collective_id=0, has_side_effects=True, vmem_limit_bytes=48 * 1024 * 1024
        ),
        name="chains",
    )(spread, left_maps[:, 0], right_maps[:, 0], top_edge, bottom_edge)


def environment_kernel(
    row_count,
    col_count,
    kets_ref,
    above_ref,
    below_ref,
    left_ref,
    right_ref,
    rows_ref,
    bonds_ref,
    ops_ref,
    energy_ref,
    near,
    far,
    vbuf,
    jbuf,
    thi,
    tlo,
    opens,
    hop_out,
    hop_in,
    half_in,
    shares,
    row_share,
    hop_send,
    hop_recv,
    half_send,
    half_recv,
    share_send,
    share_recv,
):
    local_cols = above_ref.shape[0]
    chi, width = above_ref.shape[1:]
    half = chi // 2
    rows_at = lax.axis_index("rows")
    cols_at = lax.axis_index("cols")
    has_left = cols_at > 0
    has_right = cols_at < col_count - 1
    pairs = PHYS * PHYS

    barrier = pltpu.get_barrier_semaphore()
    for other in range(row_count):

        @pl.when(rows_at != other)
        def _():
            pl.semaphore_signal(barrier, inc=1, device_id={"rows": other})

    for other in range(col_count):

        @pl.when(cols_at != other)
        def _():
            pl.semaphore_signal(barrier, inc=1, device_id={"cols": other})

    thi[...] = jnp.zeros_like(thi)
    tlo[...] = jnp.zeros_like(tlo)
    vbuf[...] = jnp.zeros_like(vbuf)
    unit = jnp.where(
        lax.broadcasted_iota(jnp.int32, (LANES, LANES), 0)
        == lax.broadcasted_iota(jnp.int32, (LANES, LANES), 1),
        1.0,
        0.0,
    ).astype(jnp.bfloat16)
    fill = jnp.zeros((LANES - chi, LANES), jnp.bfloat16)
    for column in range(local_cols):
        for source, flipped_side, is_near in ((above_ref, 0, True), (below_ref, 1, False)):
            blocks = unpack_lanes(load_tiles(source, column, width), chi)
            for at, block in enumerate(blocks):
                lanes = slice(at * LANES, (at + 1) * LANES)
                for part, values in enumerate(halves(block)):
                    tall = jnp.concatenate([values, fill], axis=0)
                    turned = dot_last(unit, tall).astype(jnp.bfloat16)
                    if is_near:
                        rows = slice(part * chi, (part + 1) * chi)
                        near[flipped_side, column, rows, lanes] = turned[:chi]
                        near[1 - flipped_side, column, rows, lanes] = values
                    else:
                        far[flipped_side, column, part, :, lanes] = turned
                        far[1 - flipped_side, column, part, :, lanes] = tall

    pl.semaphore_wait(barrier, row_count - 1 + col_count - 1)

    late = jnp.where(cols_at >= col_count // 2, 1, 0)

    def hop(side, step):
        return pltpu.make_async_remote_copy(
            hop_out.at[side],
            hop_in.at[side],
            hop_send.at[side],
            hop_recv.at[side],
            device_id={"cols": cols_at + step},
        )

    def half_copy(side):
        start, column, step = ((half, local_cols - 1, 1), (0, 0, -1))[side]
        return pltpu.make_async_remote_copy(
            opens.at[side, column, :, pl.ds(start, half)],
            half_in.at[side],
            half_send.at[side],
            half_recv.at[side],
            device_id={"cols": cols_at + step},
        )

    def put_environ(blocks):
        for at, block in enumerate(blocks):
            vbuf[at * chi : (at + 1) * chi] = block

    def walk(turn, unused):
        side = (turn // local_cols + late) % 2
        order = turn % local_cols
        column = order + side * (local_cols - 1 - 2 * order)
        first = ((side == 0) & (cols_at == 0)) | ((side == 1) & (cols_at == col_count - 1))
        final = ((side == 1) & (cols_at == 0)) | ((side == 0) & (cols_at == col_count - 1))
        ending = order == local_cols - 1

        @pl.when((order == 0) & jnp.logical_not(first))
        def _():
            pltpu.make_async_copy(hop_in.at[side], hop_in.at[side], hop_recv.at[side]).wait()
            put_environ(unpack_lanes(load_tiles(hop_in, side, width), chi))

        for at, edge in enumerate((left_ref, right_ref)):

            @pl.when((order == 0) & first & (side == at))
            def _():
                put_environ(unpack_lanes(load_tiles(edge, 0, width), chi))

        @pl.when(jnp.logical_not(ending & final))
        def _():
            v_high, v_low = halves(vbuf[...])
            f_high = far[side, column, 0]
            jbuf[...] = dot32(v_high, f_high) + (
                dot32(v_high, far[side, column, 1]) + dot32(v_low, f_high)
            )
            chunk = 16

            def ket(p, u, i, d, o):
                at = p * 16 + u * 8 + i * 4 + d * 2 + o
                return kets_ref[side, column, at : at + 1, :]

            def through(at, unused):
                start = pl.multiple_of(at * chunk, chunk)

                def joined(i, d):
                    return jbuf[pl.ds(i * chi + start, chunk), d * LANES : (d + 1) * LANES]

                for p in range(PHYS):
                    for u in range(D):
                        for o in range(D):
                            part = {}
                            for i2 in range(D):
                                for d2 in range(D):
                                    total = None
                                    for i in range(D):
                                        for d in range(D):
                                            term = ket(p, u, i, d, o) * joined(
                                                i * D + i2, d * D + d2
                                            )
                                            total = term if total is None else total + term
                                    part[i2, d2] = total
                            for q in range(PHYS):
                                for u2 in range(D):
                                    for o2 in range(D):
                                        total = None
                                        for i2 in range(D):
                                            for d2 in range(D):
                                                term = ket(q, u2, i2, d2, o2) * part[i2, d2]
                                                total = term if total is None else total + term
                                        high, low = halves(total)
                                        rows = pl.ds((u * D + u2) * LANES + start, chunk)
                                        spot = (p * PHYS + q) * D2 + o * D + o2
                                        lanes = slice(spot * LANES, (spot + 1) * LANES)
                                        thi[rows, lanes] = high
                                        tlo[rows, lanes] = low
                return unused

            lax.fori_loop(0, chi // chunk, through, 0)
            both = near[side, column]
            wide = D2 * LANES
            closed = None
            for pair in range(pairs):
                lanes = slice(pair * wide, (pair + 1) * wide)
                large = dot32(both, thi[:, lanes])
                value = large[:chi] + (large[chi:] + dot32(both[:chi], tlo[:, lanes]))
                opens[side, column, pair] = value
                if pair // PHYS == pair % PHYS:
                    closed = value if closed is None else closed + value
            square = jnp.sum(
                jnp.sum(closed * closed, axis=1, keepdims=True), axis=0, keepdims=True
            )
            closed = closed * (1.0 / jnp.sqrt(square / (chi * width) + EPSILON))
            blocks = [closed[:, d * LANES : (d + 1) * LANES] for d in range(D2)]
            put_environ(blocks)

            @pl.when(ending)
            def _():
                for t, tile in enumerate(pack_lanes(blocks, chi)):
                    hop_out[side, :, t * LANES : (t + 1) * LANES] = tile

            for at, step in enumerate((1, -1)):

                @pl.when(ending & (side == at))
                def _():
                    hop(at, step).start()
                    half_copy(at).start()

        return unused

    lax.fori_loop(0, 2 * local_cols, walk, 0)

    lane = lax.broadcasted_iota(jnp.int32, rows_ref.shape, 1)

    def density(former, latter):
        total = jnp.zeros(rows_ref.shape, jnp.float32)
        for p in range(pairs):
            mine = former(p)
            for q in range(pairs):
                value = jnp.sum(
                    jnp.sum(mine * latter(q), axis=0, keepdims=True), axis=1, keepdims=True
                )
                total = jnp.where(lane == p * pairs + q, value, total)
        return total

    def share(bond, values):
        hit = (rows_ref[...] == rows_at) & (bonds_ref[...] == bond)
        return jnp.where(hit, values, 0.0)

    mine = shares.at[cols_at]
    mine[...] = jnp.zeros_like(rows_ref, jnp.float32)
    for column in range(local_cols - 1):
        mine[...] += share(
            cols_at * local_cols + column,
            density(lambda p: opens[0, column, p], lambda q: opens[1, column + 1, q]),
        )

    def land(side):
        pltpu.make_async_copy(half_in.at[side], half_in.at[side], half_recv.at[side]).wait()

    @pl.when(has_right)
    def _():
        land(1)
        mine[...] += share(
            cols_at * local_cols + local_cols - 1,
            density(lambda p: opens[0, local_cols - 1, p, :half], lambda q: half_in[1, q]),
        )

    @pl.when(has_left)
    def _():
        land(0)
        mine[...] += share(
            cols_at * local_cols - 1,
            density(lambda p: half_in[0, p], lambda q: opens[1, 0, q, half:]),
        )

    def spread(buffer, stage, axis, place, count):
        def copies(other):
            return pltpu.make_async_remote_copy(
                buffer.at[place],
                buffer.at[place],
                share_send.at[stage, other],
                share_recv.at[stage, place],
                device_id={axis: other},
            )

        for other in range(count):

            @pl.when(place != other)
            def _():
                copies(other).start()

        for other in range(count):

            @pl.when(place != other)
            def _():
                pltpu.make_async_copy(
                    buffer.at[other], buffer.at[other], share_recv.at[stage, other]
                ).wait()

        total = buffer[0]
        for other in range(1, count):
            total += buffer[other]

        def finish():
            for other in range(count):

                @pl.when(place != other)
                def _():
                    copies(other).wait_send()

        return total, finish

    total, finish_cols = spread(shares, 0, "cols", cols_at, col_count)
    row_share[rows_at] = total
    total, finish_rows = spread(row_share, 1, "rows", rows_at, row_count)
    picked = jnp.sum(total * ops_ref[...], axis=1, keepdims=True)
    bra, ket_at = lane % pairs, lane // pairs
    diagonal = (bra // PHYS == bra % PHYS) & (ket_at // PHYS == ket_at % PHYS)
    trace = jnp.sum(
        jnp.where(diagonal & (lane < pairs * pairs), total, 0.0), axis=1, keepdims=True
    )
    size = jnp.sqrt(jnp.sum(total * total, axis=1, keepdims=True))
    energy = picked / jnp.maximum(jnp.abs(trace), 0.25 * size)
    energy_ref[...] = jnp.broadcast_to(energy, energy_ref.shape)
    finish_cols()
    finish_rows()

    @pl.when(has_right)
    def _():
        hop(0, 1).wait_send()
        half_copy(0).wait_send()

    @pl.when(has_left)
    def _():
        hop(1, -1).wait_send()
        half_copy(1).wait_send()


def term_energies(
    row_count, col_count, kets, above, below, left_edge, right_edge, rows, bonds, ops, operators
):
    local_cols, chi, width = above.shape
    tensors = kets[0].reshape((local_cols, PHYS) + (D,) * 4)
    both = jnp.stack([tensors, jnp.swapaxes(tensors, 3, 5)]).reshape(2, local_cols, -1)
    spread = jnp.broadcast_to(both[..., None], both.shape + (LANES,))
    terms = rows.shape[0]
    picked = jnp.zeros((terms, LANES), jnp.float32)
    chosen = ops[:, None, None] == jnp.arange(operators.shape[0], dtype=jnp.int32)[None, :, None]
    chosen = jnp.sum(jnp.where(chosen, operators[None], 0.0), axis=1)
    picked = jnp.pad(chosen, ((0, 0), (0, LANES - chosen.shape[1])))
    tall = (terms, LANES)
    vmem = pl.BlockSpec(memory_space=pltpu.VMEM)
    wide = D2 * LANES
    pairs = PHYS * PHYS
    dma = pltpu.SemaphoreType.DMA
    energy = pl.pallas_call(
        functools.partial(environment_kernel, row_count, col_count),
        out_shape=jax.ShapeDtypeStruct(tall, jnp.float32),
        in_specs=[vmem] * 8,
        out_specs=vmem,
        scratch_shapes=[
            pltpu.VMEM((2, local_cols, 2 * chi, wide), jnp.bfloat16),
            pltpu.VMEM((2, local_cols, 2, LANES, wide), jnp.bfloat16),
            pltpu.VMEM((D2 * chi, LANES), jnp.float32),
            pltpu.VMEM((D2 * chi, wide), jnp.float32),
            pltpu.VMEM((wide, pairs * wide), jnp.bfloat16),
            pltpu.VMEM((wide, pairs * wide), jnp.bfloat16),
            pltpu.VMEM((2, local_cols, pairs, chi, wide), jnp.float32),
            pltpu.VMEM((2, chi, width), jnp.float32),
            pltpu.VMEM((2, chi, width), jnp.float32),
            pltpu.VMEM((2, pairs, chi // 2, wide), jnp.float32),
            pltpu.VMEM((col_count,) + tall, jnp.float32),
            pltpu.VMEM((row_count,) + tall, jnp.float32),
            dma((2,)),
            dma((2,)),
            dma((2,)),
            dma((2,)),
            dma((2, max(row_count, col_count))),
            dma((2, max(row_count, col_count))),
        ],
        compiler_params=pltpu.CompilerParams(
            collective_id=1, has_side_effects=True, vmem_limit_bytes=48 * 1024 * 1024
        ),
        name="environments",
    )(
        spread,
        above,
        below,
        left_edge,
        right_edge,
        jnp.broadcast_to(rows[:, None], tall),
        jnp.broadcast_to(bonds[:, None], tall),
        picked,
    )
    return energy[:, 0]


def shards(
    kets,
    left_maps,
    right_maps,
    top_edge,
    bottom_edge,
    left_edge,
    right_edge,
    term_rows,
    term_bonds,
    term_ops,
    operators,
):
    row_count = lax.axis_size("rows")
    col_count = lax.axis_size("cols")
    outs, envs = boundary_chains(row_count, kets, left_maps, right_maps, top_edge, bottom_edge)
    energies = term_energies(
        row_count,
        col_count,
        kets,
        envs[0],
        envs[1],
        left_edge,
        right_edge,
        term_rows,
        term_bonds,
        term_ops,
        operators,
    )
    return (outs[0][None], outs[1][None], energies)


def solution(mesh):
    placed = (
        P("rows", "cols", None),
        P(None, "rows", "cols", None, None),
        P(None, "rows", "cols", None, None),
        P("cols", None, None),
        P("cols", None, None),
        P("rows", None, None),
        P("rows", None, None),
        P(),
        P(),
        P(),
        P(),
    )
    return jax.shard_map(
        shards,
        mesh=mesh,
        in_specs=placed,
        out_specs=(P("rows", "cols", None, None), P("rows", "cols", None, None), P()),
        check_vma=False,
    )
```

```python
import functools

import jax
import jax.numpy as jnp
from jax import lax
from jax.experimental import pallas as pl
from jax.experimental.pallas import tpu as pltpu
from jax.sharding import PartitionSpec as P

D = 2
D2 = 4
PHYS = 2
EPSILON = 1e-06
LANES = 128


def unpack_lanes(tiles, chi):
    rolled = {}
    lane = lax.broadcasted_iota(jnp.int32, tiles[0].shape, 1)
    blocks = []
    for block in range(D2):
        total = jnp.zeros_like(tiles[0])
        for place, tile in enumerate(tiles):
            low = max(chi * block, LANES * place)
            high = min(chi * (block + 1), LANES * (place + 1))
            if low >= high:
                continue
            shift = (LANES * place - chi * block) % LANES
            if (place, shift) not in rolled:
                rolled[place, shift] = tile if shift == 0 else pltpu.roll(tile, shift, 1)
            inside = (lane >= low - chi * block) & (lane < high - chi * block)
            total = jnp.where(inside, rolled[place, shift], total)
        blocks.append(total)
    return blocks


def pack_lanes(blocks, chi):
    lane = lax.broadcasted_iota(jnp.int32, blocks[0].shape, 1)
    rolled = {}
    tiles = []
    for place in range(chi * D2 // LANES):
        total = jnp.zeros_like(blocks[0])
        for block, values in enumerate(blocks):
            low = max(chi * block, LANES * place)
            high = min(chi * (block + 1), LANES * (place + 1))
            if low >= high:
                continue
            shift = (chi * block - LANES * place) % LANES
            if (block, shift) not in rolled:
                rolled[block, shift] = values if shift == 0 else pltpu.roll(values, shift, 1)
            inside = (lane >= low - LANES * place) & (lane < high - LANES * place)
            total = jnp.where(inside, rolled[block, shift], total)
        tiles.append(total)
    return tiles


def halves(values):
    high = values.astype(jnp.bfloat16)
    low = (values - high.astype(jnp.float32)).astype(jnp.bfloat16)
    return high, low


def dot32(former, latter):
    return jnp.dot(former, latter, preferred_element_type=jnp.float32)


def dot_last(former, latter):
    return lax.dot_general(
        former, latter, (((1,), (1,)), ((), ())), preferred_element_type=jnp.float32
    )


def load_tiles(ref, at, width):
    return [ref[at, :, LANES * t : LANES * (t + 1)] for t in range(width // LANES)]


def window_kernel(
    row_count,
    col_count,
    kets_ref,
    left_maps_ref,
    right_maps_ref,
    top_ref,
    bottom_ref,
    left_ref,
    right_ref,
    rows_ref,
    bonds_ref,
    ops_ref,
    table_ref,
    out_ref,
    energy_ref,
    kets,
    kets_env,
    maps,
    edges,
    sides,
    env_ref,
    pbuf,
    qbuf,
    kbuf,
    xbuf,
    ebuf,
    pick,
    pboth,
    qhi,
    qlo,
    x32,
    jbuf,
    thi,
    tlo,
    near,
    far,
    vbuf,
    opens,
    hop_out,
    hop_in,
    half_in,
    shares,
    row_share,
    load_sem,
    map_send,
    map_recv,
    env_send,
    env_recv,
    out_send,
    out_recv,
    chain_send,
    chain_recv,
    hop_send,
    hop_recv,
    half_send,
    half_recv,
    share_send,
    share_recv,
):
    local_cols = kets.shape[1]
    chi, width = maps.shape[3], maps.shape[4]
    half = chi // 2
    wide = D2 * LANES
    pairs = PHYS * PHYS
    terms = rows_ref.shape[1]
    tall = shares.shape[1:]
    group = 2 * local_cols
    groups = row_count // group
    place = lax.axis_index("rows")
    cols_at = lax.axis_index("cols")
    has_left = cols_at > 0
    has_right = cols_at < col_count - 1
    mine = place // group
    me = place % group
    column = me // 2
    way = me % 2
    base = mine * group
    before = mine - 1 + 2 * way
    after = mine + 1 - 2 * way
    has_before = (before >= 0) & (before < groups)
    has_after = (after >= 0) & (after < groups)

    barrier = pltpu.get_barrier_semaphore()
    for other in range(row_count):

        @pl.when(place != other)
        def _():
            pl.semaphore_signal(barrier, inc=1, device_id={"rows": other})

    for other in range(col_count):

        @pl.when(cols_at != other)
        def _():
            pl.semaphore_signal(barrier, inc=1, device_id={"cols": other})

    loads = [
        pltpu.make_async_copy(source, target, load_sem.at[at])
        for at, (source, target) in enumerate(
            (
                (right_maps_ref.at[:, 0], maps.at[0]),
                (left_maps_ref.at[:, 0], maps.at[1]),
                (top_ref, edges.at[0]),
                (bottom_ref, edges.at[1]),
                (left_ref, sides.at[pl.ds(0, 1)]),
                (right_ref, sides.at[pl.ds(1, 1)]),
            )
        )
    ]
    for load in loads:
        load.start()

    count = kets_ref.shape[2]
    spot = lax.broadcasted_iota(jnp.int32, (count, count), 0)
    from_lane = lax.broadcasted_iota(jnp.int32, (count, count), 1)

    def exchanged(high, low):
        top, bottom = (spot // high) % 2, (spot // low) % 2
        return spot + (bottom - top) * high + (top - bottom) * low

    for order, target in ((spot, 0), (exchanged(8, 2), 1), (exchanged(4, 1), 2)):
        for at in range(local_cols):
            values = jnp.broadcast_to(kets_ref[0, at : at + 1, :], (count, count))
            tallest = jnp.sum(
                jnp.where(order == from_lane, values, 0.0), axis=1, keepdims=True
            )
            filled = jnp.broadcast_to(tallest, (count, LANES))
            if target < 2:
                kets[target, at] = filled
            if target != 1:
                kets_env[target // 2, at] = filled

    chosen = lax.broadcasted_iota(jnp.int32, (wide, width), 0)
    entry = lax.broadcasted_iota(jnp.int32, (wide, width), 1)
    wanted = (chosen % LANES) * D2 + chosen // LANES
    live = (chosen % LANES) < chi
    pick[...] = jnp.where((wanted == entry) & live, 1.0, 0.0).astype(jnp.bfloat16)
    thi[...] = jnp.zeros_like(thi)
    tlo[...] = jnp.zeros_like(tlo)
    for load in loads:
        load.wait()
    pl.semaphore_wait(barrier, row_count - 1 + col_count - 1)

    def map_copies(target_way, target_col, target, local):
        made = []
        for kind, (source, buffer) in enumerate(
            ((kets, kbuf), (maps.at[0], qbuf), (maps.at[1], pbuf))
        ):
            origin, landing = source.at[target_way, target_col], buffer.at[me]
            if local:
                made.append(pltpu.make_async_copy(origin, landing, map_recv.at[kind, me]))
            else:
                made.append(
                    pltpu.make_async_remote_copy(
                        origin,
                        landing,
                        map_send.at[kind, target],
                        map_recv.at[kind, me],
                        device_id={"rows": base + target},
                    )
                )
        return made

    low_half = jnp.where(mine >= groups // 2, 1, 0)
    for turn in range(group):
        target_way = (low_half + turn // local_cols) % 2
        target_col = turn % local_cols
        target = target_col * 2 + target_way

        @pl.when(target != me)
        def _():
            for copy in map_copies(target_way, target_col, target, False):
                copy.start()

        @pl.when(target == me)
        def _():
            for copy in map_copies(target_way, target_col, target, True):
                copy.start()

    def prepare(step, unused):
        slot = step + way * (group - 1 - 2 * step)
        for kind, buffer in enumerate((kbuf, qbuf, pbuf)):
            pltpu.make_async_copy(
                buffer.at[slot], buffer.at[slot], map_recv.at[kind, slot]
            ).wait()
        ket = kbuf[slot]
        half = ket.shape[0] // PHYS
        for i in range(half):
            total = ket[i : i + 1] * ket[0:half]
            for p in range(1, PHYS):
                total += ket[p * half + i : p * half + i + 1] * ket[p * half : (p + 1) * half]
            ebuf[step, i * half : (i + 1) * half] = total
        values = pick[...]
        for source, high_ref, low_ref, right in (
            (qbuf, qhi, qlo, True),
            (pbuf, pboth, pboth, False),
        ):
            for at, (part, ref) in enumerate(zip(halves(source[slot]), (high_ref, low_ref))):
                if right:
                    fill = jnp.zeros((LANES - chi, width), jnp.bfloat16)
                    tall = dot_last(values, jnp.concatenate([part, fill], axis=0))
                    for w in range(D2):
                        ref[step, :, w * LANES : (w + 1) * LANES] = tall[
                            w * LANES : (w + 1) * LANES
                        ].astype(jnp.bfloat16)
                else:
                    spread_map = dot_last(part, values).astype(jnp.bfloat16)
                    ref[step, at * chi : (at + 1) * chi] = spread_map
        return unused

    def row_copy(source, landing, send, recv, slot):
        remote = pltpu.make_async_remote_copy(
            source, landing, send, recv, device_id={"rows": base + slot}
        )
        return remote, pltpu.make_async_copy(source, landing, recv)

    def send_row(source, landing, send, recv, slot):
        remote, local = row_copy(source, landing, send, recv, slot)

        @pl.when(slot != me)
        def _():
            remote.start()

        @pl.when(slot == me)
        def _():
            local.start()

    chain_hop = pltpu.make_async_remote_copy(
        xbuf.at[group],
        xbuf.at[0],
        chain_send,
        chain_recv,
        device_id={"rows": after * group + me},
    )

    start_slot = way * (group - 1)
    crossing = jnp.logical_not(has_before) & ((start_slot // local_cols) != (me // local_cols))
    ahead = jnp.where(has_before, group, jnp.where(crossing, group - local_cols + 1, 1))
    turned_by = jnp.where(crossing, local_cols, 0)

    def prepare_ahead(turn, unused):
        return prepare((turn + turned_by) % group, unused)

    lax.fori_loop(0, ahead, prepare_ahead, 0)

    @pl.when(has_before)
    def _():
        pltpu.make_async_copy(xbuf.at[0], xbuf.at[0], chain_recv).wait()

    @pl.when(jnp.logical_not(has_before) & (way == 0))
    def _():
        xbuf[0] = edges[0, column]

    @pl.when(jnp.logical_not(has_before) & (way == 1))
    def _():
        xbuf[0] = edges[1, column]

    for u, block in enumerate(unpack_lanes(load_tiles(xbuf, 0, width), chi)):
        x32[u * chi : (u + 1) * chi] = block

    def absorb(step, unused):
        slot = step + way * (group - 1 - 2 * step)

        pending = (step >= 1) & jnp.logical_not(crossing & (step >= local_cols))

        @pl.when(pending & jnp.logical_not(has_before))
        def _():
            prepare(step, 0)

        send_row(
            xbuf.at[step], env_ref.at[way, column], env_send.at[step], env_recv.at[way, column], slot
        )
        x_high, x_low = halves(x32[...])
        q_high = qhi[step]
        jbuf[...] = dot32(x_high, q_high) + (dot32(x_high, qlo[step]) + dot32(x_low, q_high))
        chunk = 16

        def through(at, unused):
            start = pl.multiple_of(at * chunk, chunk)
            for l in range(D2):
                for d in range(D2):
                    total = None
                    for u in range(D2):
                        for w in range(D2):
                            ket_at = (u // D) * 8 + (l // D) * 4 + (d // D) * 2 + w // D
                            bra_at = (u % D) * 8 + (l % D) * 4 + (d % D) * 2 + w % D
                            spot = ket_at * 16 + bra_at
                            term = (
                                ebuf[step, spot : spot + 1, :]
                                * jbuf[
                                    pl.ds(u * chi + start, chunk), w * LANES : (w + 1) * LANES
                                ]
                            )
                            total = term if total is None else total + term
                    high, low = halves(total)
                    rows = pl.ds(l * LANES + start, chunk)
                    thi[rows, d * LANES : (d + 1) * LANES] = high
                    tlo[rows, d * LANES : (d + 1) * LANES] = low
            return unused

        lax.fori_loop(0, chi // chunk, through, 0)
        both = pboth[step]
        large = dot32(both, thi[:, 0:wide])
        renewed = large[:chi] + (large[chi:] + dot32(both[:chi], tlo[:, 0:wide]))
        square = jnp.sum(jnp.sum(renewed * renewed, axis=1, keepdims=True), axis=0, keepdims=True)
        renewed = renewed * (1.0 / jnp.sqrt(square / (chi * width) + EPSILON))
        blocks = [renewed[:, d * LANES : (d + 1) * LANES] for d in range(D2)]
        for d, block in enumerate(blocks):
            x32[d * chi : (d + 1) * chi] = block
        for t, tile in enumerate(pack_lanes(blocks, chi)):
            xbuf[step + 1, :, t * LANES : (t + 1) * LANES] = tile

        @pl.when((step == group - 1) & has_after)
        def _():
            chain_hop.start()

        send_row(
            xbuf.at[step + 1],
            out_ref.at[way, column],
            out_send.at[step],
            out_recv.at[way, column],
            slot,
        )
        return unused

    lax.fori_loop(0, group, absorb, 0)

    unit = jnp.where(
        lax.broadcasted_iota(jnp.int32, (LANES, LANES), 0)
        == lax.broadcasted_iota(jnp.int32, (LANES, LANES), 1),
        1.0,
        0.0,
    ).astype(jnp.bfloat16)
    fill = jnp.zeros((LANES - chi, LANES), jnp.bfloat16)

    def take_boundary(kind):
        for column in range(local_cols):
            landed = env_ref.at[kind, column]
            pltpu.make_async_copy(landed, landed, env_recv.at[kind, column]).wait()
            blocks = unpack_lanes(load_tiles(env_ref.at[kind], column, width), chi)
            for at, block in enumerate(blocks):
                lanes = slice(at * LANES, (at + 1) * LANES)
                for part, values in enumerate(halves(block)):
                    tall_block = jnp.concatenate([values, fill], axis=0)
                    turned = dot_last(unit, tall_block).astype(jnp.bfloat16)
                    if kind == 0:
                        rows = slice(part * chi, (part + 1) * chi)
                        near[0, column, rows, lanes] = turned[:chi]
                        near[1, column, rows, lanes] = values
                    else:
                        far[1, column, part, :, lanes] = turned
                        far[0, column, part, :, lanes] = tall_block

    for turn in range(2):
        for kind in range(2):

            @pl.when((turn + low_half) % 2 == kind)
            def _():
                take_boundary(kind)

    spot_row = lax.broadcasted_iota(jnp.int32, (terms, terms), 0)
    spot_lane = lax.broadcasted_iota(jnp.int32, (terms, terms), 1)

    def stand(ref):
        values = jnp.broadcast_to(ref[...].astype(jnp.float32), (terms, terms))
        return jnp.sum(jnp.where(spot_row == spot_lane, values, 0.0), axis=1, keepdims=True)

    term_row = stand(rows_ref).astype(jnp.int32)
    term_bond = stand(bonds_ref).astype(jnp.int32)
    term_op = stand(ops_ref).astype(jnp.int32)
    term_weights = jnp.zeros((terms, table_ref.shape[1]), jnp.float32)
    for op in range(table_ref.shape[0]):
        term_weights = jnp.where(term_op == op, table_ref[op : op + 1, :], term_weights)

    late = jnp.where(cols_at >= col_count // 2, 1, 0)

    def hop(side, step):
        return pltpu.make_async_remote_copy(
            hop_out.at[side],
            hop_in.at[side],
            hop_send.at[side],
            hop_recv.at[side],
            device_id={"cols": cols_at + step},
        )

    def half_copy(side):
        start, column, step = ((half, local_cols - 1, 1), (0, 0, -1))[side]
        return pltpu.make_async_remote_copy(
            opens.at[side, column, :, pl.ds(start, half)],
            half_in.at[side],
            half_send.at[side],
            half_recv.at[side],
            device_id={"cols": cols_at + step},
        )

    def put_environ(blocks):
        for at, block in enumerate(blocks):
            vbuf[at * chi : (at + 1) * chi] = block

    def walk(turn, unused):
        side = (turn // local_cols + late) % 2
        order = turn % local_cols
        column = order + side * (local_cols - 1 - 2 * order)
        first = ((side == 0) & (cols_at == 0)) | ((side == 1) & (cols_at == col_count - 1))
        final = ((side == 1) & (cols_at == 0)) | ((side == 0) & (cols_at == col_count - 1))
        ending = order == local_cols - 1

        @pl.when((order == 0) & jnp.logical_not(first))
        def _():
            pltpu.make_async_copy(hop_in.at[side], hop_in.at[side], hop_recv.at[side]).wait()
            put_environ(unpack_lanes(load_tiles(hop_in, side, width), chi))

        for at in range(2):

            @pl.when((order == 0) & first & (side == at))
            def _():
                put_environ(unpack_lanes(load_tiles(sides, at, width), chi))

        @pl.when(jnp.logical_not(ending & final))
        def _():
            v_high, v_low = halves(vbuf[...])
            f_high = far[side, column, 0]
            jbuf[...] = dot32(v_high, f_high) + (
                dot32(v_high, far[side, column, 1]) + dot32(v_low, f_high)
            )
            chunk = 16

            def ket(p, u, i, d, o):
                at = p * 16 + u * 8 + i * 4 + d * 2 + o
                return kets_env[side, column, at : at + 1, :]

            def through(at, unused):
                start = pl.multiple_of(at * chunk, chunk)

                def joined(i, d):
                    return jbuf[pl.ds(i * chi + start, chunk), d * LANES : (d + 1) * LANES]

                for p in range(PHYS):
                    for u in range(D):
                        for o in range(D):
                            part = {}
                            for i2 in range(D):
                                for d2 in range(D):
                                    total = None
                                    for i in range(D):
                                        for d in range(D):
                                            term = ket(p, u, i, d, o) * joined(
                                                i * D + i2, d * D + d2
                                            )
                                            total = term if total is None else total + term
                                    part[i2, d2] = total
                            for q in range(PHYS):
                                for u2 in range(D):
                                    for o2 in range(D):
                                        total = None
                                        for i2 in range(D):
                                            for d2 in range(D):
                                                term = ket(q, u2, i2, d2, o2) * part[i2, d2]
                                                total = term if total is None else total + term
                                        high, low = halves(total)
                                        rows = pl.ds((u * D + u2) * LANES + start, chunk)
                                        spot = (p * PHYS + q) * D2 + o * D + o2
                                        lanes = slice(spot * LANES, (spot + 1) * LANES)
                                        thi[rows, lanes] = high
                                        tlo[rows, lanes] = low
                return unused

            lax.fori_loop(0, chi // chunk, through, 0)
            both = near[side, column]
            wide = D2 * LANES
            closed = None
            for pair in range(pairs):
                lanes = slice(pair * wide, (pair + 1) * wide)
                large = dot32(both, thi[:, lanes])
                value = large[:chi] + (large[chi:] + dot32(both[:chi], tlo[:, lanes]))
                opens[side, column, pair] = value
                if pair // PHYS == pair % PHYS:
                    closed = value if closed is None else closed + value
            square = jnp.sum(
                jnp.sum(closed * closed, axis=1, keepdims=True), axis=0, keepdims=True
            )
            closed = closed * (1.0 / jnp.sqrt(square / (chi * width) + EPSILON))
            blocks = [closed[:, d * LANES : (d + 1) * LANES] for d in range(D2)]
            put_environ(blocks)

            @pl.when(ending)
            def _():
                for t, tile in enumerate(pack_lanes(blocks, chi)):
                    hop_out[side, :, t * LANES : (t + 1) * LANES] = tile

            for at, step in enumerate((1, -1)):

                @pl.when(ending & (side == at))
                def _():
                    hop(at, step).start()
                    half_copy(at).start()

        return unused

    lax.fori_loop(0, 2 * local_cols, walk, 0)

    lane = lax.broadcasted_iota(jnp.int32, tall, 1)

    def density(former, latter):
        total = jnp.zeros(tall, jnp.float32)
        for p in range(pairs):
            first = former(p)
            for q in range(pairs):
                value = jnp.sum(
                    jnp.sum(first * latter(q), axis=0, keepdims=True), axis=1, keepdims=True
                )
                total = jnp.where(lane == p * pairs + q, value, total)
        return total

    def share(bond, values):
        hit = (term_row == place) & (term_bond == bond)
        return jnp.where(hit, values, 0.0)

    held = shares.at[cols_at]
    held[...] = jnp.zeros(tall, jnp.float32)
    for column in range(local_cols - 1):
        held[...] += share(
            cols_at * local_cols + column,
            density(lambda p: opens[0, column, p], lambda q: opens[1, column + 1, q]),
        )

    def land(side):
        pltpu.make_async_copy(half_in.at[side], half_in.at[side], half_recv.at[side]).wait()

    @pl.when(has_right)
    def _():
        land(1)
        held[...] += share(
            cols_at * local_cols + local_cols - 1,
            density(lambda p: opens[0, local_cols - 1, p, :half], lambda q: half_in[1, q]),
        )

    @pl.when(has_left)
    def _():
        land(0)
        held[...] += share(
            cols_at * local_cols - 1,
            density(lambda p: half_in[0, p], lambda q: opens[1, 0, q, half:]),
        )

    def spread(buffer, stage, axis, at, count):
        def copies(other):
            return pltpu.make_async_remote_copy(
                buffer.at[at],
                buffer.at[at],
                share_send.at[stage, other],
                share_recv.at[stage, at],
                device_id={axis: other},
            )

        for other in range(count):

            @pl.when(at != other)
            def _():
                copies(other).start()

        for other in range(count):

            @pl.when(at != other)
            def _():
                pltpu.make_async_copy(
                    buffer.at[other], buffer.at[other], share_recv.at[stage, other]
                ).wait()

        total = buffer[0]
        for other in range(1, count):
            total += buffer[other]

        def finish():
            for other in range(count):

                @pl.when(at != other)
                def _():
                    copies(other).wait_send()

        return total, finish

    total, finish_cols = spread(shares, 0, "cols", cols_at, col_count)
    row_share[place] = total
    total, finish_rows = spread(row_share, 1, "rows", place, row_count)
    picked = jnp.sum(total[:, : pairs * pairs] * term_weights, axis=1, keepdims=True)
    bra, ket_at = lane % pairs, lane // pairs
    diagonal = (bra // PHYS == bra % PHYS) & (ket_at // PHYS == ket_at % PHYS)
    trace = jnp.sum(
        jnp.where(diagonal & (lane < pairs * pairs), total, 0.0), axis=1, keepdims=True
    )
    size = jnp.sqrt(jnp.sum(total * total, axis=1, keepdims=True))
    energy = picked / jnp.maximum(jnp.abs(trace), 0.25 * size)
    same = lax.broadcasted_iota(jnp.int32, (terms, terms), 0) == lax.broadcasted_iota(
        jnp.int32, (terms, terms), 1
    )
    energy_ref[...] = jnp.sum(jnp.where(same, energy, 0.0), axis=0, keepdims=True)
    finish_cols()
    finish_rows()

    @pl.when(has_right)
    def _():
        hop(0, 1).wait_send()
        half_copy(0).wait_send()

    @pl.when(has_left)
    def _():
        hop(1, -1).wait_send()
        half_copy(1).wait_send()

    for step in range(group):
        slot = step + way * (group - 1 - 2 * step)

        @pl.when(slot != me)
        def _():
            row_copy(
                xbuf.at[step],
                env_ref.at[way, column],
                env_send.at[step],
                env_recv.at[way, column],
                slot,
            )[0].wait_send()
            row_copy(
                xbuf.at[step + 1],
                out_ref.at[way, column],
                out_send.at[step],
                out_recv.at[way, column],
                slot,
            )[0].wait_send()

    for target in range(group):

        @pl.when(target != me)
        def _():
            for copy in map_copies(target % 2, target // 2, target, False):
                copy.wait_send()

    @pl.when(has_after)
    def _():
        chain_hop.wait_send()

    for a in range(2):
        for b in range(local_cols):
            pltpu.make_async_copy(out_ref.at[a, b], out_ref.at[a, b], out_recv.at[a, b]).wait()


def window(row_count, col_count, args):
    local_cols = args[0].shape[1]
    chi, width = args[1].shape[-2:]
    terms = args[7].shape[0]
    group = 2 * local_cols
    wide = D2 * LANES
    pairs = PHYS * PHYS
    most = max(row_count, col_count)
    entries = args[0].shape[2]
    vmem = pl.BlockSpec(memory_space=pltpu.VMEM)
    stay = pl.BlockSpec(memory_space=pltpu.HBM)
    dma = pltpu.SemaphoreType.DMA

    def f32(*shape):
        return pltpu.VMEM(shape, jnp.float32)

    def bf16(*shape):
        return pltpu.VMEM(shape, jnp.bfloat16)

    return pl.pallas_call(
        functools.partial(window_kernel, row_count, col_count),
        out_shape=(
            jax.ShapeDtypeStruct((2, local_cols, chi, width), jnp.float32),
            jax.ShapeDtypeStruct((1, terms), jnp.float32),
        ),
        in_specs=[vmem] + [stay] * 6 + [vmem] * 4,
        out_specs=(vmem, vmem),
        scratch_shapes=[
            f32(2, local_cols, entries, LANES),
            f32(2, local_cols, entries, LANES),
            f32(2, 2, local_cols, chi, width),
            f32(2, local_cols, chi, width),
            f32(2, chi, width),
            f32(2, local_cols, chi, width),
            f32(group, chi, width),
            f32(group, chi, width),
            f32(group, entries, LANES),
            f32(group + 1, chi, width),
            f32(group, D2**4, LANES),
            bf16(wide, width),
            bf16(group, 2 * chi, wide),
            bf16(group, LANES, wide),
            bf16(group, LANES, wide),
            f32(D2 * chi, LANES),
            f32(D2 * chi, wide),
            bf16(wide, pairs * wide),
            bf16(wide, pairs * wide),
            bf16(2, local_cols, 2 * chi, wide),
            bf16(2, local_cols, 2, LANES, wide),
            f32(D2 * chi, LANES),
            f32(2, local_cols, pairs, chi, wide),
            f32(2, chi, width),
            f32(2, chi, width),
            f32(2, pairs, chi // 2, wide),
            f32(col_count, terms, LANES),
            f32(row_count, terms, LANES),
            dma((6,)),
            dma((3, group)),
            dma((3, group)),
            dma((group,)),
            dma((2, local_cols)),
            dma((group,)),
            dma((2, local_cols)),
            dma,
            dma,
            dma((2,)),
            dma((2,)),
            dma((2,)),
            dma((2,)),
            dma((2, most)),
            dma((2, most)),
        ],
        compiler_params=pltpu.CompilerParams(
            collective_id=0, has_side_effects=True, vmem_limit_bytes=56 * 1024 * 1024
        ),
        name="window",
    )(*args[:7], *(index[None] for index in args[7:10]), args[10])


def shards(*args):
    outs, energies = window(lax.axis_size("rows"), lax.axis_size("cols"), args)
    return (outs[0][None], outs[1][None], energies[0])


def solution(mesh):
    placed = (
        P("rows", "cols", None),
        P(None, "rows", "cols", None, None),
        P(None, "rows", "cols", None, None),
        P("cols", None, None),
        P("cols", None, None),
        P("rows", None, None),
        P("rows", None, None),
        P(),
        P(),
        P(),
        P(),
    )
    return jax.shard_map(
        shards,
        mesh=mesh,
        in_specs=placed,
        out_specs=(P("rows", "cols", None, None), P("rows", "cols", None, None), P()),
        check_vma=False,
    )
```
